512 devices in a mesh: gx: 8 (over z), gy: 4 (over y_hi), gz: 16 (over y_lo, x, core).
Axes of the slice: x: 4, y: 8 (y_hi: 4, y_lo: 2; y = y_hi * 2 + y_lo), z: 8, core: 2. Of those that a mesh axis runs over, the one named last changes fastest.
Arguments:
- schur: bfloat16 [8, 4, 16, 1024, 1024], P('gx', 'gy', 'gz'), may hold values from -0.2 to 2.7
- block_map: int32 [8, 4, 16, 26], P('gx', 'gy', 'gz'), may hold values from 0 to 7
- vectors: bfloat16 [8, 4, 16, 1024, 512], P('gx', 'gy', 'gz'), may hold values from -3 to 3
Outputs:
- assembled: bfloat16 [8, 4, 16, 1024, 512], P('gx', 'gy', 'gz')
- update: bfloat16 [8, 4, 16, 1024, 512], P('gx', 'gy', 'gz')
The draws below stay inside these ranges and needn't reach their ends.
All inputs are finite; a program needn't handle non-finite values.
Results may differ from the reference program's by a relative error of at most 0.0056.
Values may be sent and summed in bfloat16 or wider, within the bound.
No kernel may reach another device: no remote copies, remote signals or barrier semaphores. Data moves between devices by JAX's collectives and lax.ppermute only.
A program may use at most 64 MiB of HBM per device.

```python
import math
import jax
import jax.numpy as jnp
from jax import lax

NI = 1024
BLOCK = 128
RHS = 512
SLABS = 8
COLUMNS = 4
LAYERS = 16


def draw_schur(key, part):
    first, second = jax.random.split(key)
    full_shape = (SLABS, COLUMNS, LAYERS, NI, NI)
    spread = 1.5 / math.sqrt(NI)
    low_diag = 0.5
    high_diag = 1.5
    coupling = jnp.clip(jax.random.normal(first, full_shape, jnp.float32) * spread, -0.18, 0.18)
    leading = jax.random.uniform(second, full_shape[:4], jnp.float32, low_diag, high_diag)
    identity = jnp.eye(NI, dtype=jnp.float32)
    return (coupling + leading[..., None] * identity).astype(jnp.bfloat16)


def plant(result, stream_key, least, largest):
    longest = result.shape.index(max(result.shape))
    spots = []
    for shift in (0, 1):
        where = [jax.random.randint(jax.random.fold_in(stream_key, axis), (), 0, length) for axis, length in enumerate(result.shape)]
        where[longest] = (where[longest] + shift) % result.shape[longest]
        spots.append(tuple(where))
    return result.at[spots[0]].set(least).at[spots[1]].set(largest)


def levels(stream_key, extent, cuts, smallest, high):
    gain, own = 1.0, jax.random.fold_in(stream_key, 6)
    for position, parts in cuts:
        steps = jnp.exp(jax.random.uniform(jax.random.fold_in(own, position), (parts,), jnp.float32, smallest / len(cuts), high / len(cuts)))
        gain = gain * jnp.repeat(steps, extent[position] // parts).reshape([-1 if axis == position else 1 for axis in range(len(extent))])
    return gain


def bell_draw(key, dims, scale, bound, shards=(), kind=jnp.bfloat16):
    factor_of = levels(key, dims, shards, -0.22, 0.18) if shards else 1.0
    values = jax.random.normal(key, dims, jnp.float32) * scale * factor_of
    return jnp.minimum(jnp.maximum(values, -bound), bound).astype(kind)


def setup_inputs(seed: int = 0) -> dict:
    keys = jax.random.split(jax.random.key(seed), 4)
    schur = draw_schur(jax.random.fold_in(keys[3], 71), 0)
    block_map = plant(jax.random.randint(keys[1], (SLABS, COLUMNS, LAYERS, 26), 0, NI // BLOCK), jax.random.fold_in(keys[1], 1), 0, (NI // BLOCK) - 1).astype(jnp.int32)
    vectors = bell_draw(keys[2], (SLABS, COLUMNS, LAYERS, NI, RHS), 0.5, 3.0, ((0, 8), (1, 4), (2, 16)))
    return {"schur": schur, "block_map": block_map, "vectors": vectors}


def directions():
    return [(a, b, c) for a in (-1, 0, 1) for b in (-1, 0, 1) for c in (-1, 0, 1) if (a, b, c) != (0, 0, 0)]


def reference(schur, block_map, vectors):
    offsets = directions()
    blocks = NI // BLOCK
    total_devices = SLABS * COLUMNS * LAYERS
    flat_schur = schur.reshape(total_devices, NI, NI)
    flat_right = vectors.reshape(total_devices, NI, RHS)

    def multiply(pair):
        return jnp.dot(pair[0], pair[1], preferred_element_type=jnp.float32).astype(jnp.bfloat16)

    product = lax.map(multiply, (flat_schur, flat_right))
    tile_grid = flat_schur.reshape(total_devices, blocks, BLOCK, blocks, BLOCK)
    diagonal = jnp.stack([tile_grid[:, k, :, k, :] for k in range(blocks)], axis=1)
    payload = jnp.concatenate([diagonal, product.reshape(total_devices, blocks, BLOCK, RHS)], axis=3)
    payload_grid = payload.reshape(SLABS, COLUMNS, LAYERS, blocks, BLOCK, BLOCK + RHS)
    labels = jnp.arange(blocks, dtype=jnp.int32)

    def assemble(index):
        p = index // (COLUMNS * LAYERS)
        q = (index // LAYERS) % COLUMNS
        r = index % LAYERS
        totals = payload_grid[p, q, r].astype(jnp.float32)
        counts = jnp.ones((blocks,), jnp.float32)
        for number, (a, b, c) in enumerate(offsets):
            opposite = offsets.index((-a, -b, -c))
            near_p = (p + a) % SLABS
            near_q = q + b
            near_r = r + c
            alive = (near_q >= 0) & (near_q < COLUMNS) & (near_r >= 0) & (near_r < LAYERS)
            near_q = jnp.clip(near_q, 0, COLUMNS - 1)
            near_r = jnp.clip(near_r, 0, LAYERS - 1)
            source = block_map[near_p, near_q, near_r, opposite]
            piece = payload_grid[near_p, near_q, near_r, source].astype(jnp.float32)
            weight = ((labels == block_map[p, q, r, number]) & alive).astype(jnp.float32)
            totals = totals + weight[:, None, None] * piece[None, :, :]
            counts = counts + weight
        coupling = totals[:, :, :BLOCK]
        summed = totals[:, :, BLOCK:]
        scaled = (jnp.einsum("bij,bjk->bik", coupling, summed, precision=lax.Precision.HIGHEST) / counts[:, None, None]).astype(jnp.bfloat16)
        update = jnp.dot(flat_schur[index], scaled.reshape(NI, RHS), preferred_element_type=jnp.float32).astype(jnp.bfloat16)
        return summed.reshape(NI, RHS).astype(jnp.bfloat16), update

    assembled, update = lax.map(assemble, jnp.arange(total_devices, dtype=jnp.int32))
    return assembled.reshape(SLABS, COLUMNS, LAYERS, NI, RHS), update.reshape(SLABS, COLUMNS, LAYERS, NI, RHS)
```

```python
import functools

import jax
import jax.numpy as jnp
from jax import lax
from jax.experimental import pallas as pl
from jax.experimental.pallas import tpu as pltpu
from jax.sharding import PartitionSpec as P

BLOCK = 128
HALF = BLOCK // 2
AXES = ("gx", "gy", "gz")
STEPS = (-1, 0, 1)
SIDES = (-1, 1)


def link(a, b, c):
    place = 9 * (a + 1) + 3 * (b + 1) + (c + 1)
    return place if place < 13 else place - 1


def cell(first, second):
    return 3 * (first + 1) + (second + 1)


def shift(value, axis, step, wrap):
    count = lax.axis_size(axis)
    pairs = [
        (source, (source + step) % count)
        for source in range(count)
        if wrap or 0 <= source + step < count
    ]
    return lax.ppermute(value, axis, pairs)


def head_kernel(links, schur, vectors, payload, low_b, high_b, low_c, high_c):
    blocks = payload.shape[0]
    right_side = vectors[...]
    for k in range(blocks):
        rows = slice(k * BLOCK, (k + 1) * BLOCK)
        payload[k, :, BLOCK:] = jnp.dot(
            schur[rows, :], right_side, preferred_element_type=jnp.float32
        ).astype(jnp.bfloat16)
        payload[k, :, :BLOCK] = schur[rows, rows]
    for b, out in zip(SIDES, (low_b, high_b)):
        for a in STEPS:
            for c in STEPS:
                out[cell(a, c)] = payload[links[link(a, b, c)], :HALF, :]
    for c, out in zip(SIDES, (low_c, high_c)):
        for a in STEPS:
            for b in STEPS:
                out[cell(a, b)] = payload[links[link(a, b, c)], HALF:, :]


def first_a_kernel(links, payload, from_low_b, from_high_b, low_a, high_a):
    for a, out in zip(SIDES, (low_a, high_a)):
        for c in STEPS:
            out[cell(-1, c)] = from_low_b[cell(a, c)]
            out[cell(1, c)] = from_high_b[cell(a, c)]
            out[cell(0, c)] = payload[links[link(a, 0, c)], :HALF, :]


def first_c_kernel(links, payload, from_low_b, from_high_b, from_low_a, from_high_a, low_c, high_c):
    for c, out in zip(SIDES, (low_c, high_c)):
        for b in STEPS:
            out[cell(-1, b)] = from_low_a[cell(b, c)]
            out[cell(1, b)] = from_high_a[cell(b, c)]
        out[cell(0, -1)] = from_low_b[cell(0, c)]
        out[cell(0, 1)] = from_high_b[cell(0, c)]
        out[cell(0, 0)] = payload[links[link(0, 0, c)], :HALF, :]


def second_a_kernel(links, payload, from_low_c, from_high_c, low_a, high_a):
    for a, out in zip(SIDES, (low_a, high_a)):
        for b in STEPS:
            out[cell(b, -1)] = from_low_c[cell(a, b)]
            out[cell(b, 1)] = from_high_c[cell(a, b)]
            out[cell(b, 0)] = payload[links[link(a, b, 0)], HALF:, :]


def second_b_kernel(links, payload, from_low_c, from_high_c, from_low_a, from_high_a, low_b, high_b):
    for b, out in zip(SIDES, (low_b, high_b)):
        for c in STEPS:
            out[cell(-1, c)] = from_low_a[cell(b, c)]
            out[cell(1, c)] = from_high_a[cell(b, c)]
        out[cell(0, -1)] = from_low_c[cell(0, b)]
        out[cell(0, 1)] = from_high_c[cell(0, b)]
        out[cell(0, 0)] = payload[links[link(0, b, 0)], HALF:, :]


def add_into(totals, slot, rows, piece):
    totals[slot, rows, :] = totals[slot, rows, :] + piece.astype(jnp.float32)


def early_kernel(
    links,
    payload,
    first_low_b,
    first_high_b,
    first_low_a,
    first_high_a,
    second_low_c,
    second_high_c,
    second_low_a,
    second_high_a,
    totals,
):
    top, bottom = slice(0, HALF), slice(HALF, BLOCK)
    totals[...] = payload[...].astype(jnp.float32)
    for b, piece in zip(SIDES, (first_low_b, first_high_b)):
        add_into(totals, links[link(0, -b, 0)], top, piece[cell(0, 0)])
    for a, piece in zip(SIDES, (first_low_a, first_high_a)):
        for b in STEPS:
            add_into(totals, links[link(-a, -b, 0)], top, piece[cell(b, 0)])
    for c, piece in zip(SIDES, (second_low_c, second_high_c)):
        add_into(totals, links[link(0, 0, -c)], bottom, piece[cell(0, 0)])
    for a, piece in zip(SIDES, (second_low_a, second_high_a)):
        for c in STEPS:
            add_into(totals, links[link(-a, 0, -c)], bottom, piece[cell(0, c)])


def tail_kernel(
    columns,
    layers,
    links,
    place,
    early,
    first_low_c,
    first_high_c,
    second_low_b,
    second_high_b,
    schur,
    assembled,
    update,
    totals,
    scaled,
    counts,
):
    blocks = early.shape[0]
    top, bottom = slice(0, HALF), slice(HALF, BLOCK)
    row, layer = place[0], place[1]
    for k in range(blocks):
        counts[k] = 1
    for a in STEPS:
        for b in STEPS:
            for c in STEPS:
                if (a, b, c) == (0, 0, 0):
                    continue
                slot = links[link(a, b, c)]
                alive = (row + b >= 0) & (row + b < columns) & (layer + c >= 0) & (layer + c < layers)
                counts[slot] = counts[slot] + jnp.where(alive, 1, 0)
    totals[...] = early[...]
    for c, piece in zip(SIDES, (first_low_c, first_high_c)):
        for a in STEPS:
            for b in STEPS:
                add_into(totals, links[link(-a, -b, -c)], top, piece[cell(a, b)])
    for b, piece in zip(SIDES, (second_low_b, second_high_b)):
        for a in STEPS:
            for c in STEPS:
                add_into(totals, links[link(-a, -b, -c)], bottom, piece[cell(a, c)])
    for k in range(blocks):
        rows = slice(k * BLOCK, (k + 1) * BLOCK)
        coupling = totals[k, :, :BLOCK]
        summed = totals[k, :, BLOCK:]
        summed_high = summed.astype(jnp.bfloat16)
        summed_low = (summed - summed_high.astype(jnp.float32)).astype(jnp.bfloat16)
        coupling_high = coupling.astype(jnp.bfloat16)
        coupling_low = (coupling - coupling_high.astype(jnp.float32)).astype(jnp.bfloat16)
        assembled[rows, :] = summed_high
        mixed = jnp.dot(coupling_high, summed_high, preferred_element_type=jnp.float32)
        mixed += jnp.dot(coupling_high, summed_low, preferred_element_type=jnp.float32)
        mixed += jnp.dot(coupling_low, summed_high, preferred_element_type=jnp.float32)
        share = jnp.full((BLOCK, 1), counts[k], jnp.int32).astype(jnp.float32)
        scaled[rows, :] = (mixed / share).astype(jnp.bfloat16)
    for k in range(blocks):
        rows = slice(k * BLOCK, (k + 1) * BLOCK)
        update[rows, :] = jnp.dot(
            schur[rows, :], scaled[...], preferred_element_type=jnp.float32
        ).astype(jnp.bfloat16)


def call(kernel, name, outs, *operands, smem=1, scratch=()):
    specs = [
        pl.BlockSpec(memory_space=pltpu.SMEM if i < smem else pltpu.VMEM) for i in range(len(operands))
    ]
    return pl.pallas_call(
        kernel,
        name=name,
        out_shape=outs,
        in_specs=specs,
        out_specs=[pl.BlockSpec(memory_space=pltpu.VMEM) for _ in outs],
        scratch_shapes=list(scratch),
        compiler_params=pltpu.CompilerParams(vmem_limit_bytes=40 * 1024 * 1024),
    )(*operands)


def local(schur, block_map, vectors):
    matrix = schur[0, 0, 0]
    right_side = vectors[0, 0, 0]
    links = block_map[0, 0, 0]
    order, width = right_side.shape
    blocks = order // BLOCK
    full = BLOCK + width
    bundle = jax.ShapeDtypeStruct((9, HALF, full), jnp.bfloat16)
    place = jnp.stack([lax.axis_index("gy"), lax.axis_index("gz")]).astype(jnp.int32)

    payload, b_low, b_high, c_low, c_high = call(
        head_kernel,
        "head",
        [jax.ShapeDtypeStruct((blocks, BLOCK, full), jnp.bfloat16)] + [bundle] * 4,
        links,
        matrix,
        right_side,
    )
    first_b = [shift(v, "gy", s, False) for s, v in zip(SIDES, (b_low, b_high))]
    second_c = [shift(v, "gz", s, False) for s, v in zip(SIDES, (c_low, c_high))]
    sent = call(second_a_kernel, "second_a", [bundle] * 2, links, payload, *second_c)
    second_a = [shift(v, "gx", s, True) for s, v in zip(SIDES, sent)]
    sent = call(first_a_kernel, "first_a", [bundle] * 2, links, payload, *first_b)
    first_a = [shift(v, "gx", s, True) for s, v in zip(SIDES, sent)]
    sent = call(second_b_kernel, "second_b", [bundle] * 2, links, payload, *second_c, *second_a)
    second_b = [shift(v, "gy", s, False) for s, v in zip(SIDES, sent)]
    sent = call(first_c_kernel, "first_c", [bundle] * 2, links, payload, *first_b, *first_a)
    first_c = [shift(v, "gz", s, False) for s, v in zip(SIDES, sent)]
    (early,) = call(
        early_kernel,
        "early",
        [jax.ShapeDtypeStruct((blocks, BLOCK, full), jnp.float32)],
        links,
        payload,
        *first_b,
        *first_a,
        *second_c,
        *second_a,
    )
    assembled, update = call(
        functools.partial(tail_kernel, lax.axis_size("gy"), lax.axis_size("gz")),
        "tail",
        [jax.ShapeDtypeStruct((order, width), jnp.bfloat16)] * 2,
        links,
        place,
        early,
        *first_c,
        *second_b,
        matrix,
        smem=2,
        scratch=[
            pltpu.VMEM((blocks, BLOCK, full), jnp.float32),
            pltpu.VMEM((order, width), jnp.bfloat16),
            pltpu.SMEM((blocks,), jnp.int32),
        ],
    )
    return (assembled[None, None, None], update[None, None, None])


def solution(mesh):
    placed = (
        P("gx", "gy", "gz", None, None),
        P("gx", "gy", "gz", None),
        P("gx", "gy", "gz", None, None),
    )
    return jax.shard_map(
        local,
        mesh=mesh,
        in_specs=placed,
        out_specs=(P("gx", "gy", "gz", None, None), P("gx", "gy", "gz", None, None)),
        check_vma=False,
    )
```

```python
import functools

import jax
import jax.numpy as jnp
from jax import lax
from jax.experimental import pallas as pl
from jax.experimental.pallas import tpu as pltpu
from jax.sharding import PartitionSpec as P


BLOCK = 128
HALF = BLOCK // 2
STEPS = (-1, 0, 1)
SIDES = (-1, 1)
MIB = 1024 * 1024


def link(a, b, c):
    place = 9 * (a + 1) + 3 * (b + 1) + (c + 1)
    return place if place < 13 else place - 1


def cell(first, second):
    return 3 * (first + 1) + (second + 1)


def shift(value, axis, step, wrap):
    count = lax.axis_size(axis)
    pairs = [
        (source, (source + step) % count)
        for source in range(count)
        if wrap or 0 <= source + step < count
    ]
    return lax.ppermute(value, axis, pairs)


def head_kernel(links, matrix, right_side, top, bottom, low_c, high_c):
    for k in range(top.shape[0]):
        rows = slice(k * BLOCK, (k + 1) * BLOCK)
        product = jnp.dot(
            matrix[rows, :], right_side[...], preferred_element_type=jnp.float32
        ).astype(jnp.bfloat16)
        diagonal = matrix[rows, rows]
        top[k, :, BLOCK:] = product[:HALF]
        top[k, :, :BLOCK] = diagonal[:HALF]
        bottom[k, :, BLOCK:] = product[HALF:]
        bottom[k, :, :BLOCK] = diagonal[HALF:]
    for c, out in zip(SIDES, (low_c, high_c)):
        for a in STEPS:
            for b in STEPS:
                out[cell(a, b)] = bottom[links[link(a, b, c)]]


def first_a_kernel(links, low_links, high_links, top, from_low_b, from_high_b, low_a, high_a):
    for a, out in zip(SIDES, (low_a, high_a)):
        for c in STEPS:
            out[cell(-1, c)] = from_low_b[low_links[link(a, -1, c)]]
            out[cell(0, c)] = top[links[link(a, 0, c)]]
            out[cell(1, c)] = from_high_b[high_links[link(a, 1, c)]]


def first_c_kernel(
    links, low_links, high_links, top, from_low_b, from_high_b, from_low_a, from_high_a, low_c, high_c
):
    for c, out in zip(SIDES, (low_c, high_c)):
        for b in STEPS:
            out[cell(-1, b)] = from_low_a[cell(b, c)]
            out[cell(1, b)] = from_high_a[cell(b, c)]
        out[cell(0, -1)] = from_low_b[low_links[link(0, -1, c)]]
        out[cell(0, 0)] = top[links[link(0, 0, c)]]
        out[cell(0, 1)] = from_high_b[high_links[link(0, 1, c)]]


def second_a_kernel(links, bottom, from_low_c, from_high_c, low_a, high_a):
    for a, out in zip(SIDES, (low_a, high_a)):
        for b in STEPS:
            out[cell(b, -1)] = from_low_c[cell(a, b)]
            out[cell(b, 0)] = bottom[links[link(a, b, 0)]]
            out[cell(b, 1)] = from_high_c[cell(a, b)]


def second_b_kernel(
    links,
    low_links,
    high_links,
    bottom,
    from_low_c,
    from_high_c,
    from_low_a,
    from_high_a,
    low_b,
    high_b,
    sums,
):
    for b, out, there in zip(SIDES, (low_b, high_b), (high_links, low_links)):
        sums[...] = jnp.zeros_like(sums)
        for a, source in zip(SIDES, (from_low_a, from_high_a)):
            for c in STEPS:
                add_into(sums, there[link(-a, -b, -c)], source[cell(b, c)])
        for c, source in zip(SIDES, (from_low_c, from_high_c)):
            add_into(sums, there[link(0, -b, -c)], source[cell(0, b)])
        add_into(sums, there[link(0, -b, 0)], bottom[links[link(0, b, 0)]])
        out[...] = sums[...].astype(jnp.bfloat16)


def add_into(sums, slot, piece):
    sums[slot] = sums[slot] + piece.astype(jnp.float32)


def lower_kernel(links, bottom, from_low_c, from_high_c, from_low_a, from_high_a, lower):
    lower[...] = bottom[...].astype(jnp.float32)
    for c, source in zip(SIDES, (from_low_c, from_high_c)):
        add_into(lower, links[link(0, 0, -c)], source[cell(0, 0)])
    for a, source in zip(SIDES, (from_low_a, from_high_a)):
        for c in STEPS:
            add_into(lower, links[link(-a, 0, -c)], source[cell(0, c)])


def upper_kernel(
    links, low_links, high_links, top, from_low_b, from_high_b, from_low_a, from_high_a, upper
):
    upper[...] = top[...].astype(jnp.float32)
    for b, source, there in zip(SIDES, (from_low_b, from_high_b), (low_links, high_links)):
        add_into(upper, links[link(0, -b, 0)], source[there[link(0, b, 0)]])
    for a, source in zip(SIDES, (from_low_a, from_high_a)):
        for b in STEPS:
            add_into(upper, links[link(-a, -b, 0)], source[cell(b, 0)])


def tail_kernel(
    columns,
    layers,
    links,
    row_here,
    layer_here,
    upper,
    lower,
    first_low_c,
    first_high_c,
    second_low_b,
    second_high_b,
    schur,
    assembled,
    update,
    totals,
    scaled,
    counts,
):
    blocks = upper.shape[0]
    row, layer = row_here[0], layer_here[0]
    for k in range(blocks):
        counts[k] = 1
    for a in STEPS:
        for b in STEPS:
            for c in STEPS:
                if (a, b, c) == (0, 0, 0):
                    continue
                slot = links[link(a, b, c)]
                alive = (row + b >= 0) & (row + b < columns) & (layer + c >= 0) & (layer + c < layers)
                counts[slot] = counts[slot] + jnp.where(alive, 1, 0)
    totals[...] = upper[...]
    for c, source in zip(SIDES, (first_low_c, first_high_c)):
        for a in STEPS:
            for b in STEPS:
                add_into(totals, links[link(-a, -b, -c)], source[cell(a, b)])
    for k in range(blocks):
        rows = slice(k * BLOCK, (k + 1) * BLOCK)
        under = (
            lower[k]
            + second_low_b[k].astype(jnp.float32)
            + second_high_b[k].astype(jnp.float32)
        )
        whole = jnp.concatenate([totals[k], under], axis=0)
        coupling = whole[:, :BLOCK]
        summed = whole[:, BLOCK:]
        summed_high = summed.astype(jnp.bfloat16)
        summed_low = (summed - summed_high.astype(jnp.float32)).astype(jnp.bfloat16)
        coupling_high = coupling.astype(jnp.bfloat16)
        coupling_low = (coupling - coupling_high.astype(jnp.float32)).astype(jnp.bfloat16)
        assembled[rows, :] = summed_high
        mixed = jnp.dot(coupling_high, summed_high, preferred_element_type=jnp.float32)
        mixed += jnp.dot(coupling_high, summed_low, preferred_element_type=jnp.float32)
        mixed += jnp.dot(coupling_low, summed_high, preferred_element_type=jnp.float32)
        share = jnp.full((BLOCK, 1), counts[k], jnp.int32).astype(jnp.float32)
        scaled[rows, :] = (mixed / share).astype(jnp.bfloat16)
    for k in range(blocks):
        rows = slice(k * BLOCK, (k + 1) * BLOCK)
        update[rows, :] = jnp.dot(
            schur[rows, :], scaled[...], preferred_element_type=jnp.float32
        ).astype(jnp.bfloat16)


def call(kernel, outs, *operands, smem=1, scratch=(), room=4):
    specs = [pl.BlockSpec(memory_space=pltpu.SMEM)] * smem
    specs += [pl.BlockSpec(memory_space=pltpu.VMEM)] * (len(operands) - smem)
    return pl.pallas_call(
        kernel,
        out_shape=outs,
        in_specs=specs,
        out_specs=[pl.BlockSpec(memory_space=pltpu.VMEM) for _ in outs],
        scratch_shapes=list(scratch),
        compiler_params=pltpu.CompilerParams(vmem_limit_bytes=room * MIB),
    )(*operands)


def local(schur, block_map, vectors):
    matrix = schur[0, 0, 0]
    right_side = vectors[0, 0, 0]
    links = block_map[0, 0, 0]
    order, width = right_side.shape
    blocks = order // BLOCK
    full = BLOCK + width
    nine = [jax.ShapeDtypeStruct((9, HALF, full), jnp.bfloat16)] * 2
    eight = [jax.ShapeDtypeStruct((blocks, HALF, full), jnp.bfloat16)] * 2
    half = [jax.ShapeDtypeStruct((blocks, HALF, full), jnp.float32)]
    maps = [links] + [shift(links, "gy", s, False) for s in SIDES]
    top, bottom, *sent = call(head_kernel, eight + nine, links, matrix, right_side, room=4)
    second_c = [shift(v, "gz", s, False) for s, v in zip(SIDES, sent)]
    first_b = [shift(top, "gy", s, False) for s in SIDES]
    sent = call(second_a_kernel, nine, links, bottom, *second_c)
    second_a = [shift(v, "gx", s, True) for s, v in zip(SIDES, sent)]
    sent = call(
        second_b_kernel,
        eight,
        *maps,
        bottom,
        *second_c,
        *second_a,
        smem=3,
        scratch=[pltpu.VMEM((blocks, HALF, full), jnp.float32)],
    )
    second_b = [shift(v, "gy", s, False) for s, v in zip(SIDES, sent)]
    sent = call(first_a_kernel, nine, *maps, top, *first_b, smem=3)
    first_a = [shift(v, "gx", s, True) for s, v in zip(SIDES, sent)]
    (lower,) = call(lower_kernel, half, links, bottom, *second_c, *second_a)
    sent = call(first_c_kernel, nine, *maps, top, *first_b, *first_a, smem=3)
    first_c = [shift(v, "gz", s, False) for s, v in zip(SIDES, sent)]
    (upper,) = call(upper_kernel, half, *maps, top, *first_b, *first_a, smem=3)
    assembled, update = call(
        functools.partial(tail_kernel, lax.axis_size("gy"), lax.axis_size("gz")),
        [jax.ShapeDtypeStruct((order, width), jnp.bfloat16)] * 2,
        links,
        lax.axis_index("gy").astype(jnp.int32).reshape(1),
        lax.axis_index("gz").astype(jnp.int32).reshape(1),
        upper,
        lower,
        *first_c,
        *second_b,
        matrix,
        smem=3,
        scratch=[
            pltpu.VMEM((blocks, HALF, full), jnp.float32),
            pltpu.VMEM((order, width), jnp.bfloat16),
            pltpu.SMEM((blocks,), jnp.int32),
        ],
        room=12,
    )
    return (assembled[None, None, None], update[None, None, None])


def solution(mesh):
    placed = (
        P("gx", "gy", "gz", None, None),
        P("gx", "gy", "gz", None),
        P("gx", "gy", "gz", None, None),
    )

    return jax.shard_map(
        local,
        mesh=mesh,
        in_specs=placed,
        out_specs=(P("gx", "gy", "gz", None, None), P("gx", "gy", "gz", None, None)),
        check_vma=False,
    )
```

```python
import functools

import jax
import jax.numpy as jnp
from jax import lax
from jax.experimental import pallas as pl
from jax.experimental.pallas import tpu as pltpu
from jax.sharding import PartitionSpec as P


BLOCK = 128
HALF = BLOCK // 2
STEPS = (-1, 0, 1)
SIDES = (-1, 1)
MIB = 1024 * 1024


def link(a, b, c):
    place = 9 * (a + 1) + 3 * (b + 1) + (c + 1)
    return place if place < 13 else place - 1


def cell(first, second):
    return 3 * (first + 1) + (second + 1)


def shift(value, axis, step, wrap):
    count = lax.axis_size(axis)
    pairs = [
        (source, (source + step) % count)
        for source in range(count)
        if wrap or 0 <= source + step < count
    ]
    return lax.ppermute(value, axis, pairs)


def head_kernel(links, row_here, layer_here, matrix, right_side, top, bottom, low_a, high_a):
    for k in range(top.shape[0]):
        rows = slice(k * BLOCK, (k + 1) * BLOCK)
        product = jnp.dot(
            matrix[rows, :], right_side[...], preferred_element_type=jnp.float32
        ).astype(jnp.bfloat16)
        diagonal = matrix[rows, rows]
        top[k, :, BLOCK:] = product[:HALF]
        top[k, :, :BLOCK] = diagonal[:HALF]
        bottom[k, :, BLOCK:] = product[HALF:]
        bottom[k, :, :BLOCK] = diagonal[HALF:]
    for a, out in zip(SIDES, (low_a, high_a)):
        for b in STEPS:
            for c in STEPS:
                out[cell(b, c)] = bottom[links[link(a, b, c)]]


def first_a_kernel(links, low_links, high_links, top, from_low_b, from_high_b, low_a, high_a):
    for a, out in zip(SIDES, (low_a, high_a)):
        for c in STEPS:
            out[cell(-1, c)] = from_low_b[low_links[link(a, -1, c)]]
            out[cell(0, c)] = top[links[link(a, 0, c)]]
            out[cell(1, c)] = from_high_b[high_links[link(a, 1, c)]]


def first_c_kernel(
    links, low_links, high_links, top, from_low_b, from_high_b, from_low_a, from_high_a, low_c, high_c
):
    for c, out in zip(SIDES, (low_c, high_c)):
        for b in STEPS:
            out[cell(-1, b)] = from_low_a[cell(b, c)]
            out[cell(1, b)] = from_high_a[cell(b, c)]
        out[cell(0, -1)] = from_low_b[low_links[link(0, -1, c)]]
        out[cell(0, 0)] = top[links[link(0, 0, c)]]
        out[cell(0, 1)] = from_high_b[high_links[link(0, 1, c)]]


def second_c_kernel(links, bottom, from_low_a, from_high_a, low_c, high_c):
    for c, out in zip(SIDES, (low_c, high_c)):
        for b in STEPS:
            out[cell(-1, b)] = from_low_a[cell(b, c)]
            out[cell(0, b)] = bottom[links[link(0, b, c)]]
            out[cell(1, b)] = from_high_a[cell(b, c)]


def second_b_kernel(
    links, bottom, from_low_a, from_high_a, from_low_c, from_high_c, low_b, high_b
):
    for b, out in zip(SIDES, (low_b, high_b)):
        for a in STEPS:
            out[cell(a, -1)] = from_low_c[cell(a, b)]
            out[cell(a, 1)] = from_high_c[cell(a, b)]
        out[cell(-1, 0)] = from_low_a[cell(b, 0)]
        out[cell(0, 0)] = bottom[links[link(0, b, 0)]]
        out[cell(1, 0)] = from_high_a[cell(b, 0)]


def add_into(sums, slot, piece):
    sums[slot] = sums[slot] + piece.astype(jnp.float32)


def lower_kernel(links, bottom, from_low_a, from_high_a, from_low_c, from_high_c, lower):
    lower[...] = bottom[...].astype(jnp.float32)
    for a, source in zip(SIDES, (from_low_a, from_high_a)):
        add_into(lower, links[link(-a, 0, 0)], source[cell(0, 0)])
    for c, source in zip(SIDES, (from_low_c, from_high_c)):
        for a in STEPS:
            add_into(lower, links[link(-a, 0, -c)], source[cell(a, 0)])


def upper_kernel(
    links, low_links, high_links, top, from_low_b, from_high_b, from_low_a, from_high_a, upper
):
    upper[...] = top[...].astype(jnp.float32)
    for b, source, there in zip(SIDES, (from_low_b, from_high_b), (low_links, high_links)):
        add_into(upper, links[link(0, -b, 0)], source[there[link(0, b, 0)]])
    for a, source in zip(SIDES, (from_low_a, from_high_a)):
        for b in STEPS:
            add_into(upper, links[link(-a, -b, 0)], source[cell(b, 0)])


def tail_kernel(
    columns,
    layers,
    links,
    row_here,
    layer_here,
    upper,
    lower,
    first_low_c,
    first_high_c,
    second_low_b,
    second_high_b,
    schur,
    assembled,
    update,
    over,
    under,
    scaled,
    counts,
):
    blocks = upper.shape[0]
    row, layer = row_here[0], layer_here[0]
    for k in range(blocks):
        counts[k] = 1
    for a in STEPS:
        for b in STEPS:
            for c in STEPS:
                if (a, b, c) == (0, 0, 0):
                    continue
                slot = links[link(a, b, c)]
                alive = (row + b >= 0) & (row + b < columns) & (layer + c >= 0) & (layer + c < layers)
                counts[slot] = counts[slot] + jnp.where(alive, 1, 0)
    over[...] = upper[...]
    under[...] = lower[...]
    for c, source in zip(SIDES, (first_low_c, first_high_c)):
        for a in STEPS:
            for b in STEPS:
                add_into(over, links[link(-a, -b, -c)], source[cell(a, b)])
    for b, source in zip(SIDES, (second_low_b, second_high_b)):
        for a in STEPS:
            for c in STEPS:
                add_into(under, links[link(-a, -b, -c)], source[cell(a, c)])
    for k in range(blocks):
        rows = slice(k * BLOCK, (k + 1) * BLOCK)
        whole = jnp.concatenate([over[k], under[k]], axis=0)
        coupling = whole[:, :BLOCK]
        summed = whole[:, BLOCK:]
        summed_high = summed.astype(jnp.bfloat16)
        summed_low = (summed - summed_high.astype(jnp.float32)).astype(jnp.bfloat16)
        coupling_high = coupling.astype(jnp.bfloat16)
        coupling_low = (coupling - coupling_high.astype(jnp.float32)).astype(jnp.bfloat16)
        assembled[rows, :] = summed_high
        mixed = jnp.dot(coupling_high, summed_high, preferred_element_type=jnp.float32)
        mixed += jnp.dot(coupling_high, summed_low, preferred_element_type=jnp.float32)
        mixed += jnp.dot(coupling_low, summed_high, preferred_element_type=jnp.float32)
        share = jnp.full((BLOCK, 1), counts[k], jnp.int32).astype(jnp.float32)
        scaled[rows, :] = (mixed / share).astype(jnp.bfloat16)
    for k in range(blocks):
        rows = slice(k * BLOCK, (k + 1) * BLOCK)
        update[rows, :] = jnp.dot(
            schur[rows, :], scaled[...], preferred_element_type=jnp.float32
        ).astype(jnp.bfloat16)


def call(kernel, outs, *operands, smem=1, scratch=(), room=4):
    specs = [pl.BlockSpec(memory_space=pltpu.SMEM)] * smem
    specs += [pl.BlockSpec(memory_space=pltpu.VMEM)] * (len(operands) - smem)
    return pl.pallas_call(
        kernel,
        out_shape=outs,
        in_specs=specs,
        out_specs=[pl.BlockSpec(memory_space=pltpu.VMEM) for _ in outs],
        scratch_shapes=list(scratch),
        compiler_params=pltpu.CompilerParams(vmem_limit_bytes=room * MIB),
    )(*operands)


def local(schur, block_map, vectors):
    matrix = schur[0, 0, 0]
    right_side = vectors[0, 0, 0]
    links = block_map[0, 0, 0]
    order, width = right_side.shape
    blocks = order // BLOCK
    full = BLOCK + width
    nine = [jax.ShapeDtypeStruct((9, HALF, full), jnp.bfloat16)] * 2
    eight = [jax.ShapeDtypeStruct((blocks, HALF, full), jnp.bfloat16)] * 2
    half = [jax.ShapeDtypeStruct((blocks, HALF, full), jnp.float32)]
    here = [links] + [lax.axis_index(axis).astype(jnp.int32).reshape(1) for axis in ("gy", "gz")]
    maps = [links] + [shift(links, "gy", s, False) for s in SIDES]
    top, bottom, *sent = call(head_kernel, eight + nine, *here, matrix, right_side, smem=3)
    second_a = [shift(v, "gx", s, True) for s, v in zip(SIDES, sent)]
    first_b = [shift(top, "gy", s, False) for s in SIDES]
    sent = call(second_c_kernel, nine, links, bottom, *second_a)
    second_c = [shift(v, "gz", s, False) for s, v in zip(SIDES, sent)]
    sent = call(second_b_kernel, nine, links, bottom, *second_a, *second_c)
    second_b = [shift(v, "gy", s, False) for s, v in zip(SIDES, sent)]
    sent = call(first_a_kernel, nine, *maps, top, *first_b, smem=3)
    first_a = [shift(v, "gx", s, True) for s, v in zip(SIDES, sent)]
    (lower,) = call(lower_kernel, half, links, bottom, *second_a, *second_c)
    sent = call(first_c_kernel, nine, *maps, top, *first_b, *first_a, smem=3)
    first_c = [shift(v, "gz", s, False) for s, v in zip(SIDES, sent)]
    (upper,) = call(upper_kernel, half, *maps, top, *first_b, *first_a, smem=3)
    assembled, update = call(
        functools.partial(tail_kernel, lax.axis_size("gy"), lax.axis_size("gz")),
        [jax.ShapeDtypeStruct((order, width), jnp.bfloat16)] * 2,
        *here,
        upper,
        lower,
        *first_c,
        *second_b,
        matrix,
        smem=3,
        scratch=[
            pltpu.VMEM((blocks, HALF, full), jnp.float32),
            pltpu.VMEM((blocks, HALF, full), jnp.float32),
            pltpu.VMEM((order, width), jnp.bfloat16),
            pltpu.SMEM((blocks,), jnp.int32),
        ],
        room=12,
    )
    return (assembled[None, None, None], update[None, None, None])


def solution(mesh):
    placed = (
        P("gx", "gy", "gz", None, None),
        P("gx", "gy", "gz", None),
        P("gx", "gy", "gz", None, None),
    )

    return jax.shard_map(
        local,
        mesh=mesh,
        in_specs=placed,
        out_specs=(P("gx", "gy", "gz", None, None), P("gx", "gy", "gz", None, None)),
        check_vma=False,
    )
```

```python
import functools

import jax
import jax.numpy as jnp
from jax import lax
from jax.experimental import pallas as pl
from jax.experimental.pallas import tpu as pltpu
from jax.sharding import PartitionSpec as P


BLOCK = 128
HALF = BLOCK // 2
STEPS = (-1, 0, 1)
SIDES = (-1, 1)
MIB = 1024 * 1024


def link(a, b, c):
    place = 9 * (a + 1) + 3 * (b + 1) + (c + 1)
    return place if place < 13 else place - 1


def cell(first, second):
    return 3 * (first + 1) + (second + 1)


def shift(value, axis, step, wrap):
    count = lax.axis_size(axis)
    pairs = [
        (source, (source + step) % count)
        for source in range(count)
        if wrap or 0 <= source + step < count
    ]
    return lax.ppermute(value, axis, pairs)


def head_kernel(links, row_here, layer_here, matrix, right_side, top, bottom, low_a, high_a):
    for k in range(top.shape[0]):
        rows = slice(k * BLOCK, (k + 1) * BLOCK)
        product = jnp.dot(
            matrix[rows, :], right_side[...], preferred_element_type=jnp.float32
        ).astype(jnp.bfloat16)
        diagonal = matrix[rows, rows]
        top[k, :, BLOCK:] = product[:HALF]
        top[k, :, :BLOCK] = diagonal[:HALF]
        bottom[k, :, BLOCK:] = product[HALF:]
        bottom[k, :, :BLOCK] = diagonal[HALF:]
    for a, out in zip(SIDES, (low_a, high_a)):
        for b in STEPS:
            for c in STEPS:
                out[cell(b, c)] = bottom[links[link(a, b, c)]]


def first_a_kernel(links, low_links, high_links, top, from_low_b, from_high_b, low_a, high_a):
    for a, out in zip(SIDES, (low_a, high_a)):
        for c in STEPS:
            out[cell(-1, c)] = from_low_b[low_links[link(a, -1, c)]]
            out[cell(0, c)] = top[links[link(a, 0, c)]]
            out[cell(1, c)] = from_high_b[high_links[link(a, 1, c)]]


def first_c_kernel(
    links, low_links, high_links, top, from_low_b, from_high_b, from_low_a, from_high_a, low_c, high_c
):
    for c, out in zip(SIDES, (low_c, high_c)):
        for b in STEPS:
            out[cell(-1, b)] = from_low_a[cell(b, c)]
            out[cell(1, b)] = from_high_a[cell(b, c)]
        out[cell(0, -1)] = from_low_b[low_links[link(0, -1, c)]]
        out[cell(0, 0)] = top[links[link(0, 0, c)]]
        out[cell(0, 1)] = from_high_b[high_links[link(0, 1, c)]]


def second_b_kernel(links, bottom, from_low_a, from_high_a, low_b, high_b):
    for b, out in zip(SIDES, (low_b, high_b)):
        for c in STEPS:
            out[cell(-1, c)] = from_low_a[cell(b, c)]
            out[cell(0, c)] = bottom[links[link(0, b, c)]]
            out[cell(1, c)] = from_high_a[cell(b, c)]


def second_c_kernel(
    links, bottom, from_low_a, from_high_a, from_low_b, from_high_b, low_c, high_c
):
    for c, out in zip(SIDES, (low_c, high_c)):
        for a in STEPS:
            out[cell(a, -1)] = from_low_b[cell(a, c)]
            out[cell(a, 1)] = from_high_b[cell(a, c)]
        out[cell(-1, 0)] = from_low_a[cell(0, c)]
        out[cell(0, 0)] = bottom[links[link(0, 0, c)]]
        out[cell(1, 0)] = from_high_a[cell(0, c)]


def add_into(sums, slot, piece):
    sums[slot] = sums[slot] + piece.astype(jnp.float32)


def seed_kernel(links, bottom, from_low_a, from_high_a, lower):
    lower[...] = bottom[...].astype(jnp.float32)
    for a, source in zip(SIDES, (from_low_a, from_high_a)):
        add_into(lower, links[link(-a, 0, 0)], source[cell(0, 0)])


def lower_kernel(links, seed, from_low_b, from_high_b, lower):
    lower[...] = seed[...]
    for b, source in zip(SIDES, (from_low_b, from_high_b)):
        for a in STEPS:
            add_into(lower, links[link(-a, -b, 0)], source[cell(a, 0)])


def upper_kernel(
    links, low_links, high_links, top, from_low_b, from_high_b, from_low_a, from_high_a, upper
):
    upper[...] = top[...].astype(jnp.float32)
    for b, source, there in zip(SIDES, (from_low_b, from_high_b), (low_links, high_links)):
        add_into(upper, links[link(0, -b, 0)], source[there[link(0, b, 0)]])
    for a, source in zip(SIDES, (from_low_a, from_high_a)):
        for b in STEPS:
            add_into(upper, links[link(-a, -b, 0)], source[cell(b, 0)])


def tail_kernel(
    columns,
    layers,
    links,
    row_here,
    layer_here,
    upper,
    lower,
    first_low_c,
    first_high_c,
    second_low_c,
    second_high_c,
    schur,
    assembled,
    update,
    over,
    under,
    scaled,
    counts,
):
    blocks = upper.shape[0]
    row, layer = row_here[0], layer_here[0]
    for k in range(blocks):
        counts[k] = 1
    for a in STEPS:
        for b in STEPS:
            for c in STEPS:
                if (a, b, c) == (0, 0, 0):
                    continue
                slot = links[link(a, b, c)]
                alive = (row + b >= 0) & (row + b < columns) & (layer + c >= 0) & (layer + c < layers)
                counts[slot] = counts[slot] + jnp.where(alive, 1, 0)
    over[...] = upper[...]
    under[...] = lower[...]
    for sums, low, high in (
        (over, first_low_c, first_high_c),
        (under, second_low_c, second_high_c),
    ):
        for c, source in zip(SIDES, (low, high)):
            for a in STEPS:
                for b in STEPS:
                    add_into(sums, links[link(-a, -b, -c)], source[cell(a, b)])
    for k in range(blocks):
        rows = slice(k * BLOCK, (k + 1) * BLOCK)
        whole = jnp.concatenate([over[k], under[k]], axis=0)
        coupling = whole[:, :BLOCK]
        summed = whole[:, BLOCK:]
        summed_high = summed.astype(jnp.bfloat16)
        summed_low = (summed - summed_high.astype(jnp.float32)).astype(jnp.bfloat16)
        coupling_high = coupling.astype(jnp.bfloat16)
        coupling_low = (coupling - coupling_high.astype(jnp.float32)).astype(jnp.bfloat16)
        assembled[rows, :] = summed_high
        mixed = jnp.dot(coupling_high, summed_high, preferred_element_type=jnp.float32)
        mixed += jnp.dot(coupling_high, summed_low, preferred_element_type=jnp.float32)
        mixed += jnp.dot(coupling_low, summed_high, preferred_element_type=jnp.float32)
        share = jnp.full((BLOCK, 1), counts[k], jnp.int32).astype(jnp.float32)
        scaled[rows, :] = (mixed / share).astype(jnp.bfloat16)
    for k in range(blocks):
        rows = slice(k * BLOCK, (k + 1) * BLOCK)
        update[rows, :] = jnp.dot(
            schur[rows, :], scaled[...], preferred_element_type=jnp.float32
        ).astype(jnp.bfloat16)


def call(kernel, outs, *operands, smem=1, scratch=(), room=4):
    specs = [pl.BlockSpec(memory_space=pltpu.SMEM)] * smem
    specs += [pl.BlockSpec(memory_space=pltpu.VMEM)] * (len(operands) - smem)
    return pl.pallas_call(
        kernel,
        out_shape=outs,
        in_specs=specs,
        out_specs=[pl.BlockSpec(memory_space=pltpu.VMEM) for _ in outs],
        scratch_shapes=list(scratch),
        compiler_params=pltpu.CompilerParams(vmem_limit_bytes=room * MIB),
    )(*operands)


def local(schur, block_map, vectors):
    matrix = schur[0, 0, 0]
    right_side = vectors[0, 0, 0]
    links = block_map[0, 0, 0]
    order, width = right_side.shape
    blocks = order // BLOCK
    full = BLOCK + width
    nine = [jax.ShapeDtypeStruct((9, HALF, full), jnp.bfloat16)] * 2
    eight = [jax.ShapeDtypeStruct((blocks, HALF, full), jnp.bfloat16)] * 2
    half = [jax.ShapeDtypeStruct((blocks, HALF, full), jnp.float32)]
    here = [links] + [lax.axis_index(axis).astype(jnp.int32).reshape(1) for axis in ("gy", "gz")]
    maps = [links] + [shift(links, "gy", s, False) for s in SIDES]
    top, bottom, *sent = call(head_kernel, eight + nine, *here, matrix, right_side, smem=3)
    first_b = [shift(top, "gy", s, False) for s in SIDES]
    second_a = [shift(v, "gx", s, True) for s, v in zip(SIDES, sent)]
    sent = call(second_b_kernel, nine, links, bottom, *second_a)
    second_b = [shift(v, "gy", s, False) for s, v in zip(SIDES, sent)]
    (seed,) = call(seed_kernel, half, links, bottom, *second_a)
    sent = call(first_a_kernel, nine, *maps, top, *first_b, smem=3)
    first_a = [shift(v, "gx", s, True) for s, v in zip(SIDES, sent)]
    sent = call(first_c_kernel, nine, *maps, top, *first_b, *first_a, smem=3)
    first_c = [shift(v, "gz", s, False) for s, v in zip(SIDES, sent)]
    sent = call(second_c_kernel, nine, links, bottom, *second_a, *second_b)
    second_c = [shift(v, "gz", s, False) for s, v in zip(SIDES, sent)]
    (upper,) = call(upper_kernel, half, *maps, top, *first_b, *first_a, smem=3)
    (lower,) = call(lower_kernel, half, links, seed, *second_b)
    assembled, update = call(
        functools.partial(tail_kernel, lax.axis_size("gy"), lax.axis_size("gz")),
        [jax.ShapeDtypeStruct((order, width), jnp.bfloat16)] * 2,
        *here,
        upper,
        lower,
        *first_c,
        *second_c,
        matrix,
        smem=3,
        scratch=[
            pltpu.VMEM((blocks, HALF, full), jnp.float32),
            pltpu.VMEM((blocks, HALF, full), jnp.float32),
            pltpu.VMEM((order, width), jnp.bfloat16),
            pltpu.SMEM((blocks,), jnp.int32),
        ],
        room=12,
    )
    return (assembled[None, None, None], update[None, None, None])


def solution(mesh):
    placed = (
        P("gx", "gy", "gz", None, None),
        P("gx", "gy", "gz", None),
        P("gx", "gy", "gz", None, None),
    )

    return jax.shard_map(
        local,
        mesh=mesh,
        in_specs=placed,
        out_specs=(P("gx", "gy", "gz", None, None), P("gx", "gy", "gz", None, None)),
        check_vma=False,
    )
```

```python
import functools

import jax
import jax.numpy as jnp
from jax import lax
from jax.experimental import pallas as pl
from jax.experimental.pallas import tpu as pltpu
from jax.sharding import PartitionSpec as P


BLOCK = 128
HALF = BLOCK // 2
STEPS = (-1, 0, 1)
SIDES = (-1, 1)
MIB = 1024 * 1024


def link(a, b, c):
    place = 9 * (a + 1) + 3 * (b + 1) + (c + 1)
    return place if place < 13 else place - 1


def cell(first, second):
    return 3 * (first + 1) + (second + 1)


def shift(value, axis, step, wrap):
    count = lax.axis_size(axis)
    pairs = [
        (source, (source + step) % count)
        for source in range(count)
        if wrap or 0 <= source + step < count
    ]
    return lax.ppermute(value, axis, pairs)


def head_kernel(
    links,
    row_here,
    layer_here,
    schur,
    vectors,
    top,
    bottom,
    low_a,
    high_a,
    matrix,
    right_side,
    sems,
):
    blocks = top.shape[0]
    copies = [pltpu.make_async_copy(vectors, right_side, sems.at[blocks])]
    for k in range(blocks):
        rows = slice(k * BLOCK, (k + 1) * BLOCK)
        copies.append(pltpu.make_async_copy(schur.at[rows, :], matrix.at[rows, :], sems.at[k]))
    for copy in copies:
        copy.start()
    copies[0].wait()
    for k in range(blocks):
        rows = slice(k * BLOCK, (k + 1) * BLOCK)
        copies[k + 1].wait()
        product = jnp.dot(
            matrix[rows, :], right_side[...], preferred_element_type=jnp.float32
        ).astype(jnp.bfloat16)
        diagonal = matrix[rows, rows]
        top[k, :, BLOCK:] = product[:HALF]
        top[k, :, :BLOCK] = diagonal[:HALF]
        bottom[k, :, BLOCK:] = product[HALF:]
        bottom[k, :, :BLOCK] = diagonal[HALF:]
    for a, out in zip(SIDES, (low_a, high_a)):
        for b in STEPS:
            for c in STEPS:
                out[cell(b, c)] = bottom[links[link(a, b, c)]]


def first_a_kernel(links, low_links, high_links, top, from_low_b, from_high_b, low_a, high_a):
    for a, out in zip(SIDES, (low_a, high_a)):
        for c in STEPS:
            out[cell(-1, c)] = from_low_b[low_links[link(a, -1, c)]]
            out[cell(0, c)] = top[links[link(a, 0, c)]]
            out[cell(1, c)] = from_high_b[high_links[link(a, 1, c)]]


def ahead_c_kernel(
    links,
    low_links,
    high_links,
    top,
    bottom,
    first_low_b,
    first_high_b,
    second_low_a,
    second_high_a,
    low_c,
    high_c,
):
    for c, out in zip(SIDES, (low_c, high_c)):
        out[0] = first_low_b[low_links[link(0, -1, c)]]
        out[1] = top[links[link(0, 0, c)]]
        out[2] = first_high_b[high_links[link(0, 1, c)]]
        out[3] = second_low_a[cell(0, c)]
        out[4] = bottom[links[link(0, 0, c)]]
        out[5] = second_high_a[cell(0, c)]


def late_c_kernel(from_low, from_high, low_c, high_c):
    for c, out in zip(SIDES, (low_c, high_c)):
        for step in STEPS:
            out[step + 1] = from_low[cell(step, c)]
            out[step + 4] = from_high[cell(step, c)]


def second_b_kernel(links, bottom, from_low_a, from_high_a, low_b, high_b):
    for b, out in zip(SIDES, (low_b, high_b)):
        for c in STEPS:
            out[cell(-1, c)] = from_low_a[cell(b, c)]
            out[cell(0, c)] = bottom[links[link(0, b, c)]]
            out[cell(1, c)] = from_high_a[cell(b, c)]


def add_into(sums, slot, piece):
    sums[slot] = sums[slot] + piece.astype(jnp.float32)


def seed_kernel(links, bottom, from_low_a, from_high_a, lower):
    lower[...] = bottom[...].astype(jnp.float32)
    for a, source in zip(SIDES, (from_low_a, from_high_a)):
        add_into(lower, links[link(-a, 0, 0)], source[cell(0, 0)])


def lower_kernel(links, seed, from_low_b, from_high_b, ahead_low_c, ahead_high_c, lower):
    lower[...] = seed[...]
    for b, source in zip(SIDES, (from_low_b, from_high_b)):
        for a in STEPS:
            add_into(lower, links[link(-a, -b, 0)], source[cell(a, 0)])
    for c, source in zip(SIDES, (ahead_low_c, ahead_high_c)):
        for a in STEPS:
            add_into(lower, links[link(-a, 0, -c)], source[a + 4])


def upper_kernel(
    links,
    low_links,
    high_links,
    top,
    from_low_b,
    from_high_b,
    from_low_a,
    from_high_a,
    ahead_low_c,
    ahead_high_c,
    from_low_c,
    from_high_c,
    upper,
):
    upper[...] = top[...].astype(jnp.float32)
    for b, source, there in zip(SIDES, (from_low_b, from_high_b), (low_links, high_links)):
        add_into(upper, links[link(0, -b, 0)], source[there[link(0, b, 0)]])
    for a, source in zip(SIDES, (from_low_a, from_high_a)):
        for b in STEPS:
            add_into(upper, links[link(-a, -b, 0)], source[cell(b, 0)])
    for c, ahead, source in zip(
        SIDES, (ahead_low_c, ahead_high_c), (from_low_c, from_high_c)
    ):
        for b in STEPS:
            add_into(upper, links[link(0, -b, -c)], ahead[b + 1])
            add_into(upper, links[link(1, -b, -c)], source[b + 1])
            add_into(upper, links[link(-1, -b, -c)], source[b + 4])


def tail_kernel(
    columns,
    layers,
    links,
    row_here,
    layer_here,
    upper,
    lower,
    from_low_c,
    from_high_c,
    schur,
    assembled,
    update,
    under,
    summed_rows,
    scaled,
    update_rows,
    counts,
    sems,
):
    blocks = upper.shape[0]
    row, layer = row_here[0], layer_here[0]
    for k in range(blocks):
        counts[k] = 1
    for a in STEPS:
        for b in STEPS:
            for c in STEPS:
                if (a, b, c) == (0, 0, 0):
                    continue
                slot = links[link(a, b, c)]
                alive = (row + b >= 0) & (row + b < columns) & (layer + c >= 0) & (layer + c < layers)
                counts[slot] = counts[slot] + jnp.where(alive, 1, 0)
    under[...] = lower[...]
    for c, source in zip(SIDES, (from_low_c, from_high_c)):
        for a in STEPS:
            add_into(under, links[link(-a, 1, -c)], source[a + 1])
            add_into(under, links[link(-a, -1, -c)], source[a + 4])
    copies = []
    for k in range(blocks):
        rows = slice(k * BLOCK, (k + 1) * BLOCK)
        whole = jnp.concatenate([upper[k], under[k]], axis=0)
        coupling = whole[:, :BLOCK]
        summed = whole[:, BLOCK:]
        summed_high = summed.astype(jnp.bfloat16)
        summed_low = (summed - summed_high.astype(jnp.float32)).astype(jnp.bfloat16)
        coupling_high = coupling.astype(jnp.bfloat16)
        coupling_low = (coupling - coupling_high.astype(jnp.float32)).astype(jnp.bfloat16)
        summed_rows[rows, :] = summed_high
        copies.append(
            pltpu.make_async_copy(summed_rows.at[rows, :], assembled.at[rows, :], sems.at[k])
        )
        copies[-1].start()
        mixed = jnp.dot(coupling_high, summed_high, preferred_element_type=jnp.float32)
        mixed += jnp.dot(coupling_high, summed_low, preferred_element_type=jnp.float32)
        mixed += jnp.dot(coupling_low, summed_high, preferred_element_type=jnp.float32)
        share = jnp.full((BLOCK, 1), counts[k], jnp.int32).astype(jnp.float32)
        scaled[rows, :] = (mixed / share).astype(jnp.bfloat16)
    for k in range(blocks):
        rows = slice(k * BLOCK, (k + 1) * BLOCK)
        update_rows[rows, :] = jnp.dot(
            schur[rows, :], scaled[...], preferred_element_type=jnp.float32
        ).astype(jnp.bfloat16)
        copies.append(
            pltpu.make_async_copy(update_rows.at[rows, :], update.at[rows, :], sems.at[blocks + k])
        )
        copies[-1].start()
    for copy in copies:
        copy.wait()


def call(kernel, outs, *operands, smem=1, scratch=(), room=4, far_in=0, far_out=False):
    near = pl.BlockSpec(memory_space=pltpu.VMEM)
    far = pl.BlockSpec(memory_space=pltpu.HBM)
    specs = [pl.BlockSpec(memory_space=pltpu.SMEM)] * smem
    specs += [near] * (len(operands) - smem - far_in) + [far] * far_in
    return pl.pallas_call(
        kernel,
        out_shape=outs,
        in_specs=specs,
        out_specs=[far if far_out else near for _ in outs],
        scratch_shapes=list(scratch),
        compiler_params=pltpu.CompilerParams(vmem_limit_bytes=room * MIB),
    )(*operands)


def local(schur, block_map, vectors):
    matrix = schur[0, 0, 0]
    right_side = vectors[0, 0, 0]
    links = block_map[0, 0, 0]
    order, width = right_side.shape
    blocks = order // BLOCK
    full = BLOCK + width
    nine = [jax.ShapeDtypeStruct((9, HALF, full), jnp.bfloat16)] * 2
    six = [jax.ShapeDtypeStruct((6, HALF, full), jnp.bfloat16)] * 2
    eight = [jax.ShapeDtypeStruct((blocks, HALF, full), jnp.bfloat16)] * 2
    half = [jax.ShapeDtypeStruct((blocks, HALF, full), jnp.float32)]
    here = [links] + [lax.axis_index(axis).astype(jnp.int32).reshape(1) for axis in ("gy", "gz")]
    maps = [links] + [shift(links, "gy", s, False) for s in SIDES]
    top, bottom, *sent = call(
        head_kernel,
        eight + nine,
        *here,
        matrix,
        right_side,
        smem=3,
        far_in=2,
        scratch=[
            pltpu.VMEM((order, order), jnp.bfloat16),
            pltpu.VMEM((order, width), jnp.bfloat16),
            pltpu.SemaphoreType.DMA((blocks + 1,)),
        ],
        room=51,
    )
    first_b = [shift(top, "gy", s, False) for s in SIDES]
    second_a = [shift(v, "gx", s, True) for s, v in zip(SIDES, sent)]
    sent = call(second_b_kernel, nine, links, bottom, *second_a)
    second_b = [shift(v, "gy", s, False) for s, v in zip(SIDES, sent)]
    (seed,) = call(seed_kernel, half, links, bottom, *second_a)
    sent = call(first_a_kernel, nine, *maps, top, *first_b, smem=3)
    first_a = [shift(v, "gx", s, True) for s, v in zip(SIDES, sent)]
    sent = call(ahead_c_kernel, six, *maps, top, bottom, *first_b, *second_a, smem=3)
    ahead_c = [shift(v, "gz", s, False) for s, v in zip(SIDES, sent)]
    sent = call(late_c_kernel, six, *first_a, smem=0)
    first_c = [shift(v, "gz", s, False) for s, v in zip(SIDES, sent)]
    sent = call(late_c_kernel, six, *second_b, smem=0)
    second_c = [shift(v, "gz", s, False) for s, v in zip(SIDES, sent)]
    (lower,) = call(lower_kernel, half, links, seed, *second_b, *ahead_c)
    (upper,) = call(upper_kernel, half, *maps, top, *first_b, *first_a, *ahead_c, *first_c, smem=3)
    assembled, update = call(
        functools.partial(tail_kernel, lax.axis_size("gy"), lax.axis_size("gz")),
        [jax.ShapeDtypeStruct((order, width), jnp.bfloat16)] * 2,
        *here,
        upper,
        lower,
        *second_c,
        matrix,
        smem=3,
        scratch=[
            pltpu.VMEM((blocks, HALF, full), jnp.float32),
            pltpu.VMEM((order, width), jnp.bfloat16),
            pltpu.VMEM((order, width), jnp.bfloat16),
            pltpu.VMEM((order, width), jnp.bfloat16),
            pltpu.SMEM((blocks,), jnp.int32),
            pltpu.SemaphoreType.DMA((2 * blocks,)),
        ],
        room=12,
        far_out=True,
    )
    return (assembled[None, None, None], update[None, None, None])


def solution(mesh):
    placed = (
        P("gx", "gy", "gz", None, None),
        P("gx", "gy", "gz", None),
        P("gx", "gy", "gz", None, None),
    )

    return jax.shard_map(
        local,
        mesh=mesh,
        in_specs=placed,
        out_specs=(P("gx", "gy", "gz", None, None), P("gx", "gy", "gz", None, None)),
        check_vma=False,
    )
```

```python
import functools

import jax
import jax.numpy as jnp
from jax import lax
from jax.experimental import pallas as pl
from jax.experimental.pallas import tpu as pltpu
from jax.sharding import PartitionSpec as P


BLOCK = 128
HALF = BLOCK // 2
STEPS = (-1, 0, 1)
LINKS = 26
NOTE = 16
MIB = 1024 * 1024
AXES = ("gx", "gy", "gz")


def link(a, b, c):
    place = 9 * (a + 1) + 3 * (b + 1) + (c + 1)
    if isinstance(place, int):
        return place if place < 13 else place - 1
    return jnp.where(place < 13, place, place - 1)


def cell(first, second):
    return 3 * (first + 1) + (second + 1)


def side(here, axis):
    return 1 - 2 * (here[axis][0] % 2)


def part(stack, index):
    start = index * HALF
    if not isinstance(start, int):
        start = pl.multiple_of(start, HALF)
    return stack[pl.ds(start, HALF), :]


def swap(near, far, axis, ring):
    count = lax.axis_size(axis)
    got = []
    for value, first in ((near, 0), (far, 1)):
        pairs = []
        for low in range(first, count, 2):
            high = (low + 1) % count
            if low + 1 < count or ring:
                pairs += [(low, high), (high, low)]
        got.append(lax.ppermute(value, axis, pairs))
    return got


def head_kernel(links, x, y, z, schur, vectors, top, bottom, near_a, far_a, matrix, right_side, sems):
    blocks = bottom.shape[0]
    copies = [pltpu.make_async_copy(vectors, right_side, sems.at[blocks])]
    for k in range(blocks):
        rows = slice(k * BLOCK, (k + 1) * BLOCK)
        copies.append(pltpu.make_async_copy(schur.at[rows, :], matrix.at[rows, :], sems.at[k]))
    for copy in copies:
        copy.start()
    lane = lax.broadcasted_iota(jnp.int32, (NOTE, top.shape[1]), 1)
    note = jnp.zeros((NOTE, top.shape[1]), jnp.int32)
    for i in range(LINKS):
        note = jnp.where(lane == i, links[i], note)
    top[blocks * HALF :, :] = note.astype(jnp.float32).astype(jnp.bfloat16)
    copies[0].wait()
    for k in range(blocks):
        rows = slice(k * BLOCK, (k + 1) * BLOCK)
        copies[k + 1].wait()
        product = jnp.dot(
            matrix[rows, :], right_side[...], preferred_element_type=jnp.float32
        ).astype(jnp.bfloat16)
        diagonal = matrix[rows, rows]
        upper = slice(k * HALF, (k + 1) * HALF)
        top[upper, BLOCK:] = product[:HALF]
        top[upper, :BLOCK] = diagonal[:HALF]
        bottom[k, :, BLOCK:] = product[HALF:]
        bottom[k, :, :BLOCK] = diagonal[HALF:]
    sx = side((x, y, z), 0)
    for a, out in ((sx, near_a), (-sx, far_a)):
        for b in STEPS:
            for c in STEPS:
                out[cell(b, c)] = bottom[links[link(a, b, c)]]


def first_a_kernel(
    links, x, y, z, top, near_b, far_b, near_a, far_a, near_links, far_links, notes, sems
):
    rows = top.shape[0] - NOTE
    copies = []
    for i, (source, out) in enumerate(((near_b, near_links), (far_b, far_links))):
        notes[i] = source[rows : rows + 8, :BLOCK].astype(jnp.float32).astype(jnp.int32)
        copies.append(pltpu.make_async_copy(notes.at[i], out, sems.at[i]))
        copies[-1].start()
    sx, sy = side((x, y, z), 0), side((x, y, z), 1)
    for a, out in ((sx, near_a), (-sx, far_a)):
        for c in STEPS:
            out[cell(0, c)] = part(top, links[link(a, 0, c)])
    for copy in copies:
        copy.wait()
    for a, out in ((sx, near_a), (-sx, far_a)):
        for b, source, there in ((-sy, near_b, near_links), (sy, far_b, far_links)):
            for c in STEPS:
                out[cell(b, c)] = part(source, there[0, link(a, b, c)])


def ahead_c_kernel(
    links, x, y, z, near_links, far_links, top, bottom, near_b, far_b, near_a, far_a, near_c, far_c
):
    sx, sy, sz = side((x, y, z), 0), side((x, y, z), 1), side((x, y, z), 2)
    for c, out in ((-sz, far_c), (sz, near_c)):
        out[1] = part(top, links[link(0, 0, c)])
        out[4] = bottom[links[link(0, 0, c)]]
        for b, source, there in ((-sy, near_b, near_links), (sy, far_b, far_links)):
            out[b + 1] = part(source, there[0, link(0, b, c)])
        for a, source in ((-sx, near_a), (sx, far_a)):
            out[a + 4] = source[cell(0, c)]


def late_c_kernel(axis, x, y, z, near, far, near_c, far_c):
    step, sz = side((x, y, z), axis), side((x, y, z), 2)
    for c, out in ((-sz, far_c), (sz, near_c)):
        for motion, source in ((-step, near), (step, far)):
            for other in STEPS:
                out[3 * ((motion + 1) // 2) + other + 1] = source[cell(other, c)]


def second_b_kernel(links, x, y, z, bottom, near_a, far_a, near_b, far_b):
    sx, sy = side((x, y, z), 0), side((x, y, z), 1)
    for b, out in ((sy, near_b), (-sy, far_b)):
        for c in STEPS:
            out[cell(0, c)] = bottom[links[link(0, b, c)]]
            for a, source in ((-sx, near_a), (sx, far_a)):
                out[cell(a, c)] = source[cell(b, c)]


def add_into(sums, slot, piece):
    sums[slot] = sums[slot] + piece.astype(jnp.float32)


def seed_kernel(links, x, y, z, bottom, near_a, far_a, lower):
    sx = side((x, y, z), 0)
    lower[...] = bottom[...].astype(jnp.float32)
    for a, source in ((-sx, near_a), (sx, far_a)):
        add_into(lower, links[link(-a, 0, 0)], source[cell(0, 0)])


def lower_kernel(links, x, y, z, seed, near_b, far_b, near_ahead, far_ahead, lower):
    sy, sz = side((x, y, z), 1), side((x, y, z), 2)
    lower[...] = seed[...]
    for b, source in ((-sy, near_b), (sy, far_b)):
        for a in STEPS:
            add_into(lower, links[link(-a, -b, 0)], source[cell(a, 0)])
    for c, source in ((-sz, near_ahead), (sz, far_ahead)):
        for a in STEPS:
            add_into(lower, links[link(-a, 0, -c)], source[a + 4])


def upper_kernel(
    links,
    x,
    y,
    z,
    near_links,
    far_links,
    top,
    near_b,
    far_b,
    near_a,
    far_a,
    near_ahead,
    far_ahead,
    near_c,
    far_c,
    upper,
):
    sx, sy, sz = side((x, y, z), 0), side((x, y, z), 1), side((x, y, z), 2)
    for k in range(upper.shape[0]):
        upper[k] = part(top, k).astype(jnp.float32)
    for b, source, there in ((-sy, near_b, near_links), (sy, far_b, far_links)):
        add_into(upper, links[link(0, -b, 0)], part(source, there[0, link(0, b, 0)]))
    for a, source in ((-sx, near_a), (sx, far_a)):
        for b in STEPS:
            add_into(upper, links[link(-a, -b, 0)], source[cell(b, 0)])
    for c, ahead, source in ((-sz, near_ahead, near_c), (sz, far_ahead, far_c)):
        for b in STEPS:
            add_into(upper, links[link(0, -b, -c)], ahead[b + 1])
            add_into(upper, links[link(1, -b, -c)], source[b + 1])
            add_into(upper, links[link(-1, -b, -c)], source[b + 4])


def tail_kernel(
    columns,
    layers,
    links,
    x,
    y,
    z,
    upper,
    lower,
    near_c,
    far_c,
    schur,
    assembled,
    update,
    under,
    summed_rows,
    scaled,
    update_rows,
    counts,
    sems,
):
    blocks = upper.shape[0]
    row, layer = y[0], z[0]
    sz = side((x, y, z), 2)
    for k in range(blocks):
        counts[k] = 1
    for a in STEPS:
        for b in STEPS:
            for c in STEPS:
                if (a, b, c) == (0, 0, 0):
                    continue
                slot = links[link(a, b, c)]
                alive = (row + b >= 0) & (row + b < columns) & (layer + c >= 0) & (layer + c < layers)
                counts[slot] = counts[slot] + jnp.where(alive, 1, 0)
    under[...] = lower[...]
    for c, source in ((-sz, near_c), (sz, far_c)):
        for a in STEPS:
            add_into(under, links[link(-a, 1, -c)], source[a + 1])
            add_into(under, links[link(-a, -1, -c)], source[a + 4])
    copies = []
    for k in range(blocks):
        rows = slice(k * BLOCK, (k + 1) * BLOCK)
        whole = jnp.concatenate([upper[k], under[k]], axis=0)
        coupling = whole[:, :BLOCK]
        summed = whole[:, BLOCK:]
        summed_high = summed.astype(jnp.bfloat16)
        summed_low = (summed - summed_high.astype(jnp.float32)).astype(jnp.bfloat16)
        coupling_high = coupling.astype(jnp.bfloat16)
        coupling_low = (coupling - coupling_high.astype(jnp.float32)).astype(jnp.bfloat16)
        summed_rows[rows, :] = summed_high
        copies.append(
            pltpu.make_async_copy(summed_rows.at[rows, :], assembled.at[rows, :], sems.at[k])
        )
        copies[-1].start()
        mixed = jnp.dot(coupling_high, summed_high, preferred_element_type=jnp.float32)
        mixed += jnp.dot(coupling_high, summed_low, preferred_element_type=jnp.float32)
        mixed += jnp.dot(coupling_low, summed_high, preferred_element_type=jnp.float32)
        share = jnp.full((BLOCK, 1), counts[k], jnp.int32).astype(jnp.float32)
        scaled[rows, :] = (mixed / share).astype(jnp.bfloat16)
    for k in range(blocks):
        rows = slice(k * BLOCK, (k + 1) * BLOCK)
        update_rows[rows, :] = jnp.dot(
            schur[rows, :], scaled[...], preferred_element_type=jnp.float32
        ).astype(jnp.bfloat16)
        copies.append(
            pltpu.make_async_copy(update_rows.at[rows, :], update.at[rows, :], sems.at[blocks + k])
        )
        copies[-1].start()
    for copy in copies:
        copy.wait()


def call(kernel, outs, *operands, smem=4, scratch=(), room=4, far_in=0, far_out=False, notes=0):
    near = pl.BlockSpec(memory_space=pltpu.VMEM)
    far = pl.BlockSpec(memory_space=pltpu.HBM)
    specs = [pl.BlockSpec(memory_space=pltpu.SMEM)] * smem
    specs += [near] * (len(operands) - smem - far_in) + [far] * far_in
    return pl.pallas_call(
        kernel,
        out_shape=outs,
        in_specs=specs,
        out_specs=[far if far_out else near] * (len(outs) - notes)
        + [pl.BlockSpec(memory_space=pltpu.SMEM)] * notes,
        scratch_shapes=list(scratch),
        compiler_params=pltpu.CompilerParams(vmem_limit_bytes=room * MIB),
    )(*operands)


def local(schur, block_map, vectors):
    matrix = schur[0, 0, 0]
    right_side = vectors[0, 0, 0]
    order, width = right_side.shape
    blocks = order // BLOCK
    full = BLOCK + width
    nine = [jax.ShapeDtypeStruct((9, HALF, full), jnp.bfloat16)] * 2
    six = [jax.ShapeDtypeStruct((6, HALF, full), jnp.bfloat16)] * 2
    half = [jax.ShapeDtypeStruct((blocks, HALF, full), jnp.float32)]
    place = [lax.axis_index(axis).astype(jnp.int32).reshape(1) for axis in AXES]
    here = [block_map[0, 0, 0]] + place

    top, bottom, *sent = call(
        head_kernel,
        [
            jax.ShapeDtypeStruct((blocks * HALF + NOTE, full), jnp.bfloat16),
            jax.ShapeDtypeStruct((blocks, HALF, full), jnp.bfloat16),
        ]
        + nine,
        *here,
        matrix,
        right_side,
        far_in=2,
        scratch=[
            pltpu.VMEM((order, order), jnp.bfloat16),
            pltpu.VMEM((order, width), jnp.bfloat16),
            pltpu.SemaphoreType.DMA((blocks + 1,)),
        ],
        room=51,
    )
    first_b = swap(top, top, "gy", False)
    second_a = swap(*sent, "gx", True)
    sent = call(second_b_kernel, nine, *here, bottom, *second_a)
    second_b = swap(*sent, "gy", False)
    (seed,) = call(seed_kernel, half, *here, bottom, *second_a)
    *sent, near_links, far_links = call(
        first_a_kernel,
        nine + [jax.ShapeDtypeStruct((8, BLOCK), jnp.int32)] * 2,
        *here,
        top,
        *first_b,
        scratch=[pltpu.VMEM((2, 8, BLOCK), jnp.int32), pltpu.SemaphoreType.DMA((2,))],
        notes=2,
    )
    first_a = swap(*sent, "gx", True)
    maps = [*here, near_links, far_links]
    sent = call(ahead_c_kernel, six, *maps, top, bottom, *first_b, *second_a, smem=6)
    ahead_c = swap(*sent, "gz", False)
    sent = call(functools.partial(late_c_kernel, 0), six, *place, *first_a, smem=3)
    first_c = swap(*sent, "gz", False)
    sent = call(functools.partial(late_c_kernel, 1), six, *place, *second_b, smem=3)
    second_c = swap(*sent, "gz", False)
    (lower,) = call(lower_kernel, half, *here, seed, *second_b, *ahead_c)
    (upper,) = call(upper_kernel, half, *maps, top, *first_b, *first_a, *ahead_c, *first_c, smem=6)
    assembled, update = call(
        functools.partial(tail_kernel, lax.axis_size("gy"), lax.axis_size("gz")),
        [jax.ShapeDtypeStruct((order, width), jnp.bfloat16)] * 2,
        *here,
        upper,
        lower,
        *second_c,
        matrix,
        scratch=[
            pltpu.VMEM((blocks, HALF, full), jnp.float32),
            pltpu.VMEM((order, width), jnp.bfloat16),
            pltpu.VMEM((order, width), jnp.bfloat16),
            pltpu.VMEM((order, width), jnp.bfloat16),
            pltpu.SMEM((blocks,), jnp.int32),
            pltpu.SemaphoreType.DMA((2 * blocks,)),
        ],
        room=12,
        far_out=True,
    )
    return (assembled[None, None, None], update[None, None, None])


def solution(mesh):
    placed = (
        P("gx", "gy", "gz", None, None),
        P("gx", "gy", "gz", None),
        P("gx", "gy", "gz", None, None),
    )

    return jax.shard_map(
        local,
        mesh=mesh,
        in_specs=placed,
        out_specs=(P("gx", "gy", "gz", None, None), P("gx", "gy", "gz", None, None)),
        check_vma=False,
    )
```

```python
import functools

import jax
import jax.numpy as jnp
from jax import lax
from jax.experimental import pallas as pl
from jax.experimental.pallas import tpu as pltpu
from jax.sharding import PartitionSpec as P


BLOCK = 128
HALF = BLOCK // 2
STEPS = (-1, 0, 1)
LINKS = 26
NOTE = 16
MIB = 1024 * 1024
AXES = ("gx", "gy", "gz")


def link(a, b, c):
    place = 9 * (a + 1) + 3 * (b + 1) + (c + 1)
    if isinstance(place, int):
        return place if place < 13 else place - 1
    return jnp.where(place < 13, place, place - 1)


def cell(first, second):
    return 3 * (first + 1) + (second + 1)


def side(here, axis):
    return 1 - 2 * (here[axis][0] % 2)


def part(stack, index):
    start = index * HALF
    if not isinstance(start, int):
        start = pl.multiple_of(start, HALF)
    return stack[pl.ds(start, HALF), :]


def swap(near, far, axis, ring):
    count = lax.axis_size(axis)
    got = []
    for value, first in ((near, 0), (far, 1)):
        pairs = []
        for low in range(first, count, 2):
            high = (low + 1) % count
            if low + 1 < count or ring:
                pairs += [(low, high), (high, low)]
        got.append(lax.ppermute(value, axis, pairs))
    return got


def head_kernel(links, x, y, z, schur, vectors, top, bottom, near_a, far_a, matrix, right_side, sems):
    blocks = bottom.shape[0]
    depth = vectors.shape[0] // 4
    groups = [slice(i * depth, (i + 1) * depth) for i in range(4)]
    copies = []
    for i, rows in enumerate(groups):
        copies.append(
            pltpu.make_async_copy(vectors.at[rows, :], right_side.at[rows, :], sems.at[4 + i])
        )
    for i, rows in enumerate(groups):
        copies.append(pltpu.make_async_copy(schur.at[rows, :], matrix.at[rows, :], sems.at[i]))
    for copy in copies:
        copy.start()
    lane = lax.broadcasted_iota(jnp.int32, (NOTE, top.shape[1]), 1)
    note = jnp.zeros((NOTE, top.shape[1]), jnp.int32)
    for i in range(LINKS):
        note = jnp.where(lane == i, links[i], note)
    top[blocks * HALF :, :] = note.astype(jnp.float32).astype(jnp.bfloat16)
    for copy in copies[:4]:
        copy.wait()
    for i, group in enumerate(groups):
        copies[4 + i].wait()
        product = jnp.dot(
            matrix[group, :], right_side[...], preferred_element_type=jnp.float32
        ).astype(jnp.bfloat16)
        for j in range(depth // BLOCK):
            k = i * (depth // BLOCK) + j
            rows = slice(k * BLOCK, (k + 1) * BLOCK)
            diagonal = matrix[rows, rows]
            upper = slice(k * HALF, (k + 1) * HALF)
            top[upper, BLOCK:] = product[j * BLOCK : j * BLOCK + HALF]
            top[upper, :BLOCK] = diagonal[:HALF]
            bottom[k, :, BLOCK:] = product[j * BLOCK + HALF : (j + 1) * BLOCK]
            bottom[k, :, :BLOCK] = diagonal[HALF:]
    sx = side((x, y, z), 0)
    for a, out in ((sx, near_a), (-sx, far_a)):
        for b in STEPS:
            for c in STEPS:
                out[cell(b, c)] = bottom[links[link(a, b, c)]]


def first_a_kernel(
    links, x, y, z, top, near_b, far_b, near_a, far_a, near_links, far_links, notes, sems
):
    rows = top.shape[0] - NOTE
    copies = []
    for i, (source, out) in enumerate(((near_b, near_links), (far_b, far_links))):
        notes[i] = source[rows : rows + 8, :BLOCK].astype(jnp.float32).astype(jnp.int32)
        copies.append(pltpu.make_async_copy(notes.at[i], out, sems.at[i]))
        copies[-1].start()
    sx, sy = side((x, y, z), 0), side((x, y, z), 1)
    for a, out in ((sx, near_a), (-sx, far_a)):
        for c in STEPS:
            out[cell(0, c)] = part(top, links[link(a, 0, c)])
    for copy in copies:
        copy.wait()
    for a, out in ((sx, near_a), (-sx, far_a)):
        for b, source, there in ((-sy, near_b, near_links), (sy, far_b, far_links)):
            for c in STEPS:
                out[cell(b, c)] = part(source, there[0, link(a, b, c)])


def ahead_c_kernel(
    links, x, y, z, near_links, far_links, top, bottom, near_b, far_b, near_a, far_a, near_c, far_c
):
    sx, sy, sz = side((x, y, z), 0), side((x, y, z), 1), side((x, y, z), 2)
    for c, out in ((-sz, far_c), (sz, near_c)):
        out[1] = part(top, links[link(0, 0, c)])
        out[4] = bottom[links[link(0, 0, c)]]
        for b, source, there in ((-sy, near_b, near_links), (sy, far_b, far_links)):
            out[b + 1] = part(source, there[0, link(0, b, c)])
        for a, source in ((-sx, near_a), (sx, far_a)):
            out[a + 4] = source[cell(0, c)]


def late_c_kernel(axis, x, y, z, near, far, near_c, far_c):
    step, sz = side((x, y, z), axis), side((x, y, z), 2)
    for c, out in ((-sz, far_c), (sz, near_c)):
        for motion, source in ((-step, near), (step, far)):
            for other in STEPS:
                out[3 * ((motion + 1) // 2) + other + 1] = source[cell(other, c)]


def second_b_kernel(links, x, y, z, bottom, near_a, far_a, near_b, far_b):
    sx, sy = side((x, y, z), 0), side((x, y, z), 1)
    for b, out in ((sy, near_b), (-sy, far_b)):
        for c in STEPS:
            out[cell(0, c)] = bottom[links[link(0, b, c)]]
            for a, source in ((-sx, near_a), (sx, far_a)):
                out[cell(a, c)] = source[cell(b, c)]


def add_into(sums, slot, piece):
    sums[slot] = sums[slot] + piece.astype(jnp.float32)


def seed_kernel(links, x, y, z, bottom, near_a, far_a, lower):
    sx = side((x, y, z), 0)
    lower[...] = bottom[...].astype(jnp.float32)
    for a, source in ((-sx, near_a), (sx, far_a)):
        add_into(lower, links[link(-a, 0, 0)], source[cell(0, 0)])


def lower_kernel(links, x, y, z, seed, near_b, far_b, near_ahead, far_ahead, lower):
    sy, sz = side((x, y, z), 1), side((x, y, z), 2)
    lower[...] = seed[...]
    for b, source in ((-sy, near_b), (sy, far_b)):
        for a in STEPS:
            add_into(lower, links[link(-a, -b, 0)], source[cell(a, 0)])
    for c, source in ((-sz, near_ahead), (sz, far_ahead)):
        for a in STEPS:
            add_into(lower, links[link(-a, 0, -c)], source[a + 4])


def upper_kernel(
    links,
    x,
    y,
    z,
    near_links,
    far_links,
    top,
    near_b,
    far_b,
    near_a,
    far_a,
    near_ahead,
    far_ahead,
    near_c,
    far_c,
    upper,
):
    sx, sy, sz = side((x, y, z), 0), side((x, y, z), 1), side((x, y, z), 2)
    for k in range(upper.shape[0]):
        upper[k] = part(top, k).astype(jnp.float32)
    for b, source, there in ((-sy, near_b, near_links), (sy, far_b, far_links)):
        add_into(upper, links[link(0, -b, 0)], part(source, there[0, link(0, b, 0)]))
    for a, source in ((-sx, near_a), (sx, far_a)):
        for b in STEPS:
            add_into(upper, links[link(-a, -b, 0)], source[cell(b, 0)])
    for c, ahead, source in ((-sz, near_ahead, near_c), (sz, far_ahead, far_c)):
        for b in STEPS:
            add_into(upper, links[link(0, -b, -c)], ahead[b + 1])
            add_into(upper, links[link(1, -b, -c)], source[b + 1])
            add_into(upper, links[link(-1, -b, -c)], source[b + 4])


def tail_kernel(
    columns,
    layers,
    links,
    x,
    y,
    z,
    upper,
    lower,
    near_c,
    far_c,
    schur,
    assembled,
    update,
    under,
    summed_rows,
    scaled,
    update_rows,
    counts,
    sems,
):
    blocks = upper.shape[0]
    row, layer = y[0], z[0]
    sz = side((x, y, z), 2)
    for k in range(blocks):
        counts[k] = 1
    for a in STEPS:
        for b in STEPS:
            for c in STEPS:
                if (a, b, c) == (0, 0, 0):
                    continue
                slot = links[link(a, b, c)]
                alive = (row + b >= 0) & (row + b < columns) & (layer + c >= 0) & (layer + c < layers)
                counts[slot] = counts[slot] + jnp.where(alive, 1, 0)
    under[...] = lower[...]
    for c, source in ((-sz, near_c), (sz, far_c)):
        for a in STEPS:
            add_into(under, links[link(-a, 1, -c)], source[a + 1])
            add_into(under, links[link(-a, -1, -c)], source[a + 4])
    copies = []
    for k in range(blocks):
        rows = slice(k * BLOCK, (k + 1) * BLOCK)
        whole = jnp.concatenate([upper[k], under[k]], axis=0)
        coupling = whole[:, :BLOCK]
        summed = whole[:, BLOCK:]
        summed_high = summed.astype(jnp.bfloat16)
        summed_low = (summed - summed_high.astype(jnp.float32)).astype(jnp.bfloat16)
        coupling_high = coupling.astype(jnp.bfloat16)
        coupling_low = (coupling - coupling_high.astype(jnp.float32)).astype(jnp.bfloat16)
        summed_rows[rows, :] = summed_high
        copies.append(
            pltpu.make_async_copy(summed_rows.at[rows, :], assembled.at[rows, :], sems.at[k])
        )
        copies[-1].start()
        mixed = jnp.dot(coupling_high, summed_high, preferred_element_type=jnp.float32)
        mixed += jnp.dot(coupling_high, summed_low, preferred_element_type=jnp.float32)
        mixed += jnp.dot(coupling_low, summed_high, preferred_element_type=jnp.float32)
        share = jnp.full((BLOCK, 1), counts[k], jnp.int32).astype(jnp.float32)
        scaled[rows, :] = (mixed / share).astype(jnp.bfloat16)
    for k in range(blocks):
        rows = slice(k * BLOCK, (k + 1) * BLOCK)
        update_rows[rows, :] = jnp.dot(
            schur[rows, :], scaled[...], preferred_element_type=jnp.float32
        ).astype(jnp.bfloat16)
        copies.append(
            pltpu.make_async_copy(update_rows.at[rows, :], update.at[rows, :], sems.at[blocks + k])
        )
        copies[-1].start()
    for copy in copies:
        copy.wait()


def call(kernel, outs, *operands, smem=4, scratch=(), room=4, far_in=0, far_out=False, notes=0):
    near = pl.BlockSpec(memory_space=pltpu.VMEM)
    far = pl.BlockSpec(memory_space=pltpu.HBM)
    specs = [pl.BlockSpec(memory_space=pltpu.SMEM)] * smem
    specs += [near] * (len(operands) - smem - far_in) + [far] * far_in
    return pl.pallas_call(
        kernel,
        out_shape=outs,
        in_specs=specs,
        out_specs=[far if far_out else near] * (len(outs) - notes)
        + [pl.BlockSpec(memory_space=pltpu.SMEM)] * notes,
        scratch_shapes=list(scratch),
        compiler_params=pltpu.CompilerParams(vmem_limit_bytes=room * MIB),
    )(*operands)


def local(schur, block_map, vectors):
    matrix = schur[0, 0, 0]
    right_side = vectors[0, 0, 0]
    order, width = right_side.shape
    blocks = order // BLOCK
    full = BLOCK + width
    nine = [jax.ShapeDtypeStruct((9, HALF, full), jnp.bfloat16)] * 2
    six = [jax.ShapeDtypeStruct((6, HALF, full), jnp.bfloat16)] * 2
    half = [jax.ShapeDtypeStruct((blocks, HALF, full), jnp.float32)]
    place = [lax.axis_index(axis).astype(jnp.int32).reshape(1) for axis in AXES]
    here = [block_map[0, 0, 0]] + place

    top, bottom, *sent = call(
        head_kernel,
        [
            jax.ShapeDtypeStruct((blocks * HALF + NOTE, full), jnp.bfloat16),
            jax.ShapeDtypeStruct((blocks, HALF, full), jnp.bfloat16),
        ]
        + nine,
        *here,
        matrix,
        right_side,
        far_in=2,
        scratch=[
            pltpu.VMEM((order, order), jnp.bfloat16),
            pltpu.VMEM((order, width), jnp.bfloat16),
            pltpu.SemaphoreType.DMA((blocks + 1,)),
        ],
        room=51,
    )
    first_b = swap(top, top, "gy", False)
    second_a = swap(*sent, "gx", True)
    sent = call(second_b_kernel, nine, *here, bottom, *second_a)
    second_b = swap(*sent, "gy", False)
    (seed,) = call(seed_kernel, half, *here, bottom, *second_a)
    *sent, near_links, far_links = call(
        first_a_kernel,
        nine + [jax.ShapeDtypeStruct((8, BLOCK), jnp.int32)] * 2,
        *here,
        top,
        *first_b,
        scratch=[pltpu.VMEM((2, 8, BLOCK), jnp.int32), pltpu.SemaphoreType.DMA((2,))],
        notes=2,
    )
    first_a = swap(*sent, "gx", True)
    maps = [*here, near_links, far_links]
    sent = call(ahead_c_kernel, six, *maps, top, bottom, *first_b, *second_a, smem=6)
    ahead_c = swap(*sent, "gz", False)
    sent = call(functools.partial(late_c_kernel, 0), six, *place, *first_a, smem=3)
    first_c = swap(*sent, "gz", False)
    sent = call(functools.partial(late_c_kernel, 1), six, *place, *second_b, smem=3)
    second_c = swap(*sent, "gz", False)
    (lower,) = call(lower_kernel, half, *here, seed, *second_b, *ahead_c)
    (upper,) = call(upper_kernel, half, *maps, top, *first_b, *first_a, *ahead_c, *first_c, smem=6)
    assembled, update = call(
        functools.partial(tail_kernel, lax.axis_size("gy"), lax.axis_size("gz")),
        [jax.ShapeDtypeStruct((order, width), jnp.bfloat16)] * 2,
        *here,
        upper,
        lower,
        *second_c,
        matrix,
        scratch=[
            pltpu.VMEM((blocks, HALF, full), jnp.float32),
            pltpu.VMEM((order, width), jnp.bfloat16),
            pltpu.VMEM((order, width), jnp.bfloat16),
            pltpu.VMEM((order, width), jnp.bfloat16),
            pltpu.SMEM((blocks,), jnp.int32),
            pltpu.SemaphoreType.DMA((2 * blocks,)),
        ],
        room=12,
        far_out=True,
    )
    return (assembled[None, None, None], update[None, None, None])


def solution(mesh):
    placed = (
        P("gx", "gy", "gz", None, None),
        P("gx", "gy", "gz", None),
        P("gx", "gy", "gz", None, None),
    )

    return jax.shard_map(
        local,
        mesh=mesh,
        in_specs=placed,
        out_specs=(P("gx", "gy", "gz", None, None), P("gx", "gy", "gz", None, None)),
        check_vma=False,
    )
```
